32 devices in a mesh: coarse: 2 (over y), fine: 4 (over z), model: 4 (over x, core).
Axes of the slice: x: 2, y: 2, z: 4, core: 2. Of those that a mesh axis runs over, the one named last changes fastest.
Arguments:
- fresh_keys: bfloat16 [8, 12288, 8, 128], P(None, ('coarse', 'fine'), 'model'), may hold values from -6 to 6
- fresh_values: bfloat16 [8, 12288, 8, 128], P(None, ('coarse', 'fine'), 'model'), may hold values from -6 to 6
- turn_angle: float32 [12288, 64], replicated, may hold values from -3.140625 to 3.140625
Outputs:
- cache_keys: bfloat16 [8, 12288, 8, 128], P(('coarse', 'fine'), None, 'model')
- cache_values: bfloat16 [8, 12288, 8, 128], P(('coarse', 'fine'), None, 'model')
- page_high: bfloat16 [8, 384, 8, 128], P(('coarse', 'fine'), None, 'model')
- page_low: bfloat16 [8, 384, 8, 128], P(('coarse', 'fine'), None, 'model')
The draws below stay inside these ranges and needn't reach their ends.
All inputs are finite; a program needn't handle non-finite values.
Results may differ from the reference program's by a relative error of at most 0.001.
Values may be sent and summed in bfloat16 or wider, within the bound.
A program may use at most 128 MiB of HBM per device.

```python
import jax
import jax.numpy as jnp

BATCH = 8
LENGTH = 12288
KV_HEADS = 8
HEAD_SIZE = 128
HALF_HEAD = 64
PAGE = 32


def block_levels(rng, shape, shards, least, largest):
    def one(dim, blocks):
        heights = jax.random.uniform(jax.random.fold_in(jax.random.fold_in(rng, 6), dim), (blocks,), jnp.float32, least / len(shards), largest / len(shards))
        return jnp.repeat(jnp.exp(heights), shape[dim] // blocks).reshape((-1,) + (1,) * (len(shape) - dim - 1))

    factor_of = one(*shards[0])
    for cut in shards[1:]:
        factor_of = factor_of * one(*cut)
    return factor_of


def normal_values(key, dims, width, reach, split=(), kind=jnp.bfloat16):
    array = jax.random.normal(key, dims, jnp.float32) * width
    if len(split) > 0:
        array = block_levels(key, dims, split, -0.22, 0.18) * array
    return jnp.clip(array, min=-reach, max=reach).astype(kind)


def setup_inputs(seed: int = 0) -> dict:
    streams_of = jax.random.split(jax.random.key(seed), 4)
    fresh_keys = normal_values(streams_of[0], (BATCH, LENGTH, KV_HEADS, HEAD_SIZE), 1.0, 6.0, ((1, 8), (2, 4)))
    fresh_values = normal_values(streams_of[1], (BATCH, LENGTH, KV_HEADS, HEAD_SIZE), 1.0, 6.0, ((1, 8), (2, 4)))
    turn_angle = jnp.clip(jax.random.uniform(streams_of[2], (LENGTH, HALF_HEAD), jnp.float32, -3.140625, 3.140625), -3.140625, 3.140625)
    return {"fresh_keys": fresh_keys, "fresh_values": fresh_values, "turn_angle": turn_angle}


def turn_pairs(vectors, angle):
    half = vectors.shape[-1] // 2
    cosine, sine = jnp.cos(angle)[None, :, None, :], jnp.sin(angle)[None, :, None, :]
    first, second = vectors[..., :half], vectors[..., half:]
    return jnp.concatenate([first * cosine - second * sine, second * cosine + first * sine], axis=-1)


def prepare_keys(plain_keys, angle):
    wide_keys = plain_keys.astype(jnp.float32)
    return turn_pairs(wide_keys, angle)


def reference(fresh_keys, fresh_values, turn_angle):
    turned_keys = prepare_keys(fresh_keys, turn_angle)
    narrow_keys = turned_keys.astype(jnp.bfloat16)
    page_view = narrow_keys.reshape(BATCH, LENGTH // PAGE, PAGE, KV_HEADS, HEAD_SIZE)
    page_high = jnp.max(page_view, axis=2)
    page_low = jnp.min(page_view, axis=2)
    cache_keys = narrow_keys
    cache_values = fresh_values
    return cache_keys, cache_values, page_high, page_low
```

```python
import functools

import jax
import jax.numpy as jnp
from jax import lax
from jax.experimental import pallas as pl
from jax.experimental.pallas import tpu as pltpu
from jax.sharding import PartitionSpec as P

PAGE = 32
BLOCK = 256
TILE = 16
AXES = ("coarse", "fine")
MESH = pl.DeviceIdType.MESH


def exchange_kernel(
    nc, nf, heads, keys, values, angles,
    got_keys, got_values, high, low,
    plain, turned, near_angles, cosine, sine, folded, paired,
    angle_sem, plain_sem, own_sem, key_send, key_recv, value_send, value_recv,
):
    n = nc * nf
    per, rows = keys.shape[0] // n, keys.shape[1]
    length, half = rows // heads, angles.shape[0]
    head_size = 2 * half
    mine_c, mine_f = lax.axis_index("coarse"), lax.axis_index("fine")
    me = mine_c * nf + mine_f
    my_rows = pl.ds(pl.multiple_of(me * rows, rows), rows)

    way = 1 - 2 * (mine_f // max(nf // 2, 1))

    def device(step_c, step_f):
        c = lax.rem(mine_c + step_c, nc)
        f = lax.rem(mine_f + way * step_f + nf, nf)
        return c, f, c * nf + f

    order = [(c, f) for f in list(range(1, nf)) for c in range(nc)]
    order[nc:nc] = [(c, 0) for c in range(1, nc)]
    early = nc

    angle_copy = pltpu.make_async_copy(
        angles.at[:, pl.ds(pl.multiple_of(me * length, length), length)], near_angles, angle_sem
    )
    angle_copy.start()

    def chunk_of(index):
        return pl.ds(index * per, per)

    def plain_copy(slot, index):
        return pltpu.make_async_copy(keys.at[chunk_of(index)], plain.at[slot], plain_sem.at[slot])

    partners = [device(*step) for step in order]
    for slot, (_, _, index) in enumerate(partners):
        plain_copy(slot, index).start()
    plain_copy(n - 1, me).start()

    barrier = pltpu.get_barrier_semaphore()
    for c, f, _ in partners:
        pl.semaphore_signal(barrier, inc=1, device_id={"coarse": c, "fine": f}, device_id_type=MESH)
    pl.semaphore_wait(barrier, n - 1)

    def send_values(slot):
        c, f, index = partners[slot]
        return pltpu.make_async_remote_copy(
            src_ref=values.at[chunk_of(index)],
            dst_ref=got_values.at[:, my_rows],
            send_sem=value_send.at[slot],
            recv_sem=value_recv.at[me],
            device_id={"coarse": c, "fine": f},
            device_id_type=MESH,
        )

    def send_keys(slot):
        c, f, _ = partners[slot]
        return pltpu.make_async_remote_copy(
            src_ref=turned.at[slot],
            dst_ref=got_keys.at[:, my_rows],
            send_sem=key_send.at[slot],
            recv_sem=key_recv.at[me],
            device_id={"coarse": c, "fine": f},
            device_id_type=MESH,
        )

    for slot in range(early):
        send_values(slot).start()
    own_copy = pltpu.make_async_copy(values.at[chunk_of(me)], got_values.at[:, my_rows], own_sem)
    own_copy.start()

    angle_copy.wait()
    cos_half = jnp.cos(near_angles[...]).T
    sin_half = jnp.sin(near_angles[...]).T
    cos_whole = jnp.concatenate([cos_half, cos_half], axis=1)
    sin_whole = jnp.concatenate([-sin_half, sin_half], axis=1)
    for h in range(heads):
        cosine[pl.ds(h, length, stride=heads), :] = cos_whole
        sine[pl.ds(h, length, stride=heads), :] = sin_whole

    def turn(slot, store):
        for s in range(per):
            @pl.loop(0, rows // BLOCK)
            def _(i):
                here = pl.ds(pl.multiple_of(i * BLOCK, BLOCK), BLOCK)
                wide = plain[slot, s, here, :].astype(jnp.float32)
                out = wide * cosine[here, :] + pltpu.roll(wide, half, 1) * sine[here, :]
                store(s, i, out.astype(jnp.bfloat16))

    def store_turned(slot):
        def store(s, i, block):
            turned[slot, s, pl.ds(pl.multiple_of(i * BLOCK, BLOCK), BLOCK), :] = block
        return store

    def store_own(s, i, block):
        got_keys[s, pl.ds(pl.multiple_of(me * rows + i * BLOCK, BLOCK), BLOCK), :] = block

    def prepare(slot, index):
        plain_copy(slot, index).wait()
        turn(slot, store_turned(slot))

    for slot in range(early):
        prepare(slot, partners[slot][2])
        if slot >= 1:
            send_keys(slot - 1).start()
    prepare(early, partners[early][2])
    send_keys(early - 1).start()
    for slot in range(early, n - 1):
        send_values(slot).start()
    for slot in range(early + 1, n - 1):
        prepare(slot, partners[slot][2])
        send_keys(slot - 1).start()
    plain_copy(n - 1, me).wait()
    turn(n - 1, store_own)
    send_keys(n - 2).start()

    pages = length // PAGE
    fold = PAGE * heads // TILE

    def bound(index, pick, out):
        for s in range(per):
            block = got_keys[s, pl.ds(pl.multiple_of(index * rows, rows), rows), :]
            tiles = block.reshape(pages, fold, TILE, head_size)
            best = tiles[:, 0]
            for t in range(1, fold):
                best = pick(best, tiles[:, t])
            folded[...] = best.astype(jnp.float32).reshape(pages * TILE, head_size)
            for h in range(heads):
                top = folded[pl.ds(h, pages, stride=TILE), :]
                for j in range(1, TILE // heads):
                    top = pick(top, folded[pl.ds(j * heads + h, pages, stride=TILE), :])
                paired[pl.ds(h, pages, stride=heads), :] = top
            span = pages * heads
            out[s, pl.ds(pl.multiple_of(index * span, span), span), :] = paired[...].astype(jnp.bfloat16)

    bound(me, jnp.maximum, high)
    bound(me, jnp.minimum, low)

    def arrived(buffer, sems, index):
        there = buffer.at[:, pl.ds(pl.multiple_of(index * rows, rows), rows)]
        return pltpu.make_async_copy(there, there, sems.at[index])

    def source(step_c, step_f):
        f = lax.rem(mine_f + step_f, nf)
        return lax.rem(mine_c + step_c, nc) * nf + f

    others = [source((nc - c) % nc, f) for f, c in [(f, c) for f in range(nf) for c in range(nc)][1:]]
    for index in others:
        arrived(got_keys, key_recv, index).wait()
        bound(index, jnp.maximum, high)
        bound(index, jnp.minimum, low)
    for index in others:
        arrived(got_values, value_recv, index).wait()
    own_copy.wait()
    for slot in range(n - 1):
        send_values(slot).wait_send()
        send_keys(slot).wait_send()


def write_kernel(*refs):
    count = len(refs) // 2
    sources, targets, sems = refs[:count], refs[count:2 * count], refs[2 * count]
    copies = [
        pltpu.make_async_copy(a, b, sems.at[i]) for i, (a, b) in enumerate(zip(sources, targets))
    ]
    for copy in copies:
        copy.start()
    for copy in copies:
        copy.wait()


def on_device(nc, nf, fresh_keys, fresh_values, turn_angle):
    batch, length, heads, size = fresh_keys.shape
    n, rows, half = nc * nf, length * heads, size // 2
    per = batch // n
    pages = length // PAGE
    keys = fresh_keys.reshape(batch, rows, size)
    values = fresh_values.reshape(batch, rows, size)
    whole = (per, n * rows, size)
    bounds = (per, n * pages * heads, size)
    vmem, anywhere = pl.BlockSpec(memory_space=pltpu.VMEM), pl.BlockSpec(memory_space=pl.ANY)
    arrived = pl.pallas_call(
        functools.partial(exchange_kernel, nc, nf, heads),
        out_shape=[pltpu.VMEM(shape, jnp.bfloat16) for shape in (whole, whole, bounds, bounds)],
        in_specs=[anywhere] * 3,
        out_specs=[vmem] * 4,
        scratch_shapes=[
            pltpu.VMEM((n, per, rows, size), jnp.bfloat16),
            pltpu.VMEM((n - 1, per, rows, size), jnp.bfloat16),
            pltpu.VMEM((half, length), jnp.float32),
            pltpu.VMEM((rows, size), jnp.float32),
            pltpu.VMEM((rows, size), jnp.float32),
            pltpu.VMEM((pages * TILE, size), jnp.float32),
            pltpu.VMEM((pages * heads, size), jnp.float32),
            pltpu.SemaphoreType.DMA(()),
            pltpu.SemaphoreType.DMA((n,)),
            pltpu.SemaphoreType.DMA(()),
            pltpu.SemaphoreType.DMA((n - 1,)),
            pltpu.SemaphoreType.DMA((n,)),
            pltpu.SemaphoreType.DMA((n - 1,)),
            pltpu.SemaphoreType.DMA((n,)),
        ],
        compiler_params=pltpu.CompilerParams(
            collective_id=0, has_side_effects=True, vmem_limit_bytes=40 * 2**20
        ),
        name="exchange",
    )(keys, values, turn_angle.T)
    out = pl.pallas_call(
        write_kernel,
        out_shape=[jax.ShapeDtypeStruct(a.shape, a.dtype) for a in arrived],
        in_specs=[vmem] * 4,
        out_specs=[anywhere] * 4,
        scratch_shapes=[pltpu.SemaphoreType.DMA((4,))],
        compiler_params=pltpu.CompilerParams(vmem_limit_bytes=2**20),
        name="write",
    )(*[pltpu.with_memory_space_constraint(a, pltpu.VMEM) for a in arrived])
    return tuple(a.reshape(per, -1, heads, size) for a in out)


def solution(mesh):
    where = P(AXES, None, "model", None)
    return jax.shard_map(
        functools.partial(on_device, mesh.shape["coarse"], mesh.shape["fine"]),
        mesh=mesh,
        in_specs=(P(None, AXES, "model", None), P(None, AXES, "model", None), P()),
        out_specs=(where, where, where, where),
        check_vma=False,
    )
```

```python
import functools

import jax
import jax.numpy as jnp
from jax import lax
from jax.experimental import pallas as pl
from jax.experimental.pallas import tpu as pltpu
from jax.sharding import PartitionSpec as P

PAGE = 32
BLOCK = 256
PIECE = 192
TILE = 16
AXES = ("coarse", "fine")
MESH = pl.DeviceIdType.MESH


def exchange_kernel(
    nc, nf, heads, keys, values, angles,
    got_keys, got_values, high, low,
    plain, turned, near_angles, cosine, sine, folded, paired,
    angle_sem, plain_sem, own_sem, key_send, key_recv, value_send, value_recv,
):
    n = nc * nf
    per, rows = keys.shape[0] // n, keys.shape[1]
    length, half = rows // heads, angles.shape[0]
    head_size = 2 * half
    mine_c, mine_f = lax.axis_index("coarse"), lax.axis_index("fine")
    me = mine_c * nf + mine_f
    my_rows = pl.ds(pl.multiple_of(me * rows, rows), rows)

    order = [(c, f) for f in range(nf) for c in range(nc)][1:]

    def device(step_c, step_f):
        c, f = lax.rem(mine_c + step_c, nc), lax.rem(mine_f + step_f, nf)
        return c, f, c * nf + f

    angle_copy = pltpu.make_async_copy(
        angles.at[:, pl.ds(pl.multiple_of(me * length, length), length)], near_angles, angle_sem
    )
    angle_copy.start()

    def chunk_of(index):
        return pl.ds(index * per, per)

    def plain_copy(slot, index):
        return pltpu.make_async_copy(keys.at[chunk_of(index)], plain.at[slot], plain_sem.at[slot])

    partners = [device(*step) for step in order]
    for slot, (_, _, index) in enumerate(partners):
        plain_copy(slot, index).start()
    plain_copy(n - 1, me).start()

    barrier = pltpu.get_barrier_semaphore()
    for c, f, _ in partners:
        pl.semaphore_signal(barrier, inc=1, device_id={"coarse": c, "fine": f}, device_id_type=MESH)
    pl.semaphore_wait(barrier, n - 1)

    def send(source, target, sends, recvs, slot, first, count):
        c, f, _ = partners[slot]
        return pltpu.make_async_remote_copy(
            src_ref=source.at[:, pl.ds(first, count)],
            dst_ref=target.at[:, pl.ds(pl.multiple_of(me * rows + first, PIECE), count)],
            send_sem=sends.at[slot],
            recv_sem=recvs.at[me],
            device_id={"coarse": c, "fine": f},
            device_id_type=MESH,
        )

    def send_values(slot, first, count):
        source = values.at[chunk_of(partners[slot][2])]
        return send(source, got_values, value_send, value_recv, slot, first, count)

    def send_keys(slot, first, count):
        return send(turned.at[slot], got_keys, key_send, key_recv, slot, first, count)

    pieces = rows // PIECE

    def send_pieces(send_one, first, last):
        @pl.loop(first, last)
        def _(p):
            for slot in range(n - 1):
                send_one(slot, pl.multiple_of(p * PIECE, PIECE), PIECE).start()

    send_pieces(send_values, 0, pieces // 2)
    own_copy = pltpu.make_async_copy(values.at[chunk_of(me)], got_values.at[:, my_rows], own_sem)
    own_copy.start()

    angle_copy.wait()
    cos_half = jnp.cos(near_angles[...]).T
    sin_half = jnp.sin(near_angles[...]).T
    cos_whole = jnp.concatenate([cos_half, cos_half], axis=1)
    sin_whole = jnp.concatenate([-sin_half, sin_half], axis=1)
    for h in range(heads):
        cosine[pl.ds(h, length, stride=heads), :] = cos_whole
        sine[pl.ds(h, length, stride=heads), :] = sin_whole

    def turn(slot, store):
        for s in range(per):
            @pl.loop(0, rows // BLOCK)
            def _(i):
                here = pl.ds(pl.multiple_of(i * BLOCK, BLOCK), BLOCK)
                wide = plain[slot, s, here, :].astype(jnp.float32)
                out = wide * cosine[here, :] + pltpu.roll(wide, half, 1) * sine[here, :]
                store(s, i, out.astype(jnp.bfloat16))

    def store_turned(slot):
        def store(s, i, block):
            turned[slot, s, pl.ds(pl.multiple_of(i * BLOCK, BLOCK), BLOCK), :] = block
        return store

    def store_own(s, i, block):
        got_keys[s, pl.ds(pl.multiple_of(me * rows + i * BLOCK, BLOCK), BLOCK), :] = block

    for slot, (_, _, index) in enumerate(partners):
        plain_copy(slot, index).wait()
        turn(slot, store_turned(slot))
    plain_copy(n - 1, me).wait()
    turn(n - 1, store_own)
    send_pieces(send_keys, 0, pieces)
    send_pieces(send_values, pieces // 2, pieces)

    pages = length // PAGE
    fold = PAGE * heads // TILE

    def bound(index, pick, out):
        for s in range(per):
            block = got_keys[s, pl.ds(pl.multiple_of(index * rows, rows), rows), :]
            tiles = block.reshape(pages, fold, TILE, head_size)
            best = tiles[:, 0]
            for t in range(1, fold):
                best = pick(best, tiles[:, t])
            folded[...] = best.astype(jnp.float32).reshape(pages * TILE, head_size)
            for h in range(heads):
                top = folded[pl.ds(h, pages, stride=TILE), :]
                for j in range(1, TILE // heads):
                    top = pick(top, folded[pl.ds(j * heads + h, pages, stride=TILE), :])
                paired[pl.ds(h, pages, stride=heads), :] = top
            span = pages * heads
            out[s, pl.ds(pl.multiple_of(index * span, span), span), :] = paired[...].astype(jnp.bfloat16)

    bound(me, jnp.maximum, high)
    bound(me, jnp.minimum, low)

    def arrived(buffer, sems, index):
        there = buffer.at[:, pl.ds(pl.multiple_of(index * rows, rows), rows)]
        return pltpu.make_async_copy(there, there, sems.at[index])

    others = [device((nc - c) % nc, (nf - f) % nf)[2] for c, f in order]
    for index in others:
        arrived(got_keys, key_recv, index).wait()
        bound(index, jnp.maximum, high)
        bound(index, jnp.minimum, low)
    for index in others:
        arrived(got_values, value_recv, index).wait()
    own_copy.wait()
    for slot in range(n - 1):
        send_values(slot, 0, rows).wait_send()
        send_keys(slot, 0, rows).wait_send()


def write_kernel(*refs):
    count = len(refs) // 2
    sources, targets, sems = refs[:count], refs[count:2 * count], refs[2 * count]
    copies = [
        pltpu.make_async_copy(a, b, sems.at[i]) for i, (a, b) in enumerate(zip(sources, targets))
    ]
    for copy in copies:
        copy.start()
    for copy in copies:
        copy.wait()


def on_device(nc, nf, fresh_keys, fresh_values, turn_angle):
    batch, length, heads, size = fresh_keys.shape
    n, rows, half = nc * nf, length * heads, size // 2
    per = batch // n
    pages = length // PAGE
    keys = fresh_keys.reshape(batch, rows, size)
    values = fresh_values.reshape(batch, rows, size)
    whole = (per, n * rows, size)
    bounds = (per, n * pages * heads, size)
    vmem, anywhere = pl.BlockSpec(memory_space=pltpu.VMEM), pl.BlockSpec(memory_space=pl.ANY)
    arrived = pl.pallas_call(
        functools.partial(exchange_kernel, nc, nf, heads),
        out_shape=[pltpu.VMEM(shape, jnp.bfloat16) for shape in (whole, whole, bounds, bounds)],
        in_specs=[anywhere] * 3,
        out_specs=[vmem] * 4,
        scratch_shapes=[
            pltpu.VMEM((n, per, rows, size), jnp.bfloat16),
            pltpu.VMEM((n - 1, per, rows, size), jnp.bfloat16),
            pltpu.VMEM((half, length), jnp.float32),
            pltpu.VMEM((rows, size), jnp.float32),
            pltpu.VMEM((rows, size), jnp.float32),
            pltpu.VMEM((pages * TILE, size), jnp.float32),
            pltpu.VMEM((pages * heads, size), jnp.float32),
            pltpu.SemaphoreType.DMA(()),
            pltpu.SemaphoreType.DMA((n,)),
            pltpu.SemaphoreType.DMA(()),
            pltpu.SemaphoreType.DMA((n - 1,)),
            pltpu.SemaphoreType.DMA((n,)),
            pltpu.SemaphoreType.DMA((n - 1,)),
            pltpu.SemaphoreType.DMA((n,)),
        ],
        compiler_params=pltpu.CompilerParams(
            collective_id=0, has_side_effects=True, vmem_limit_bytes=40 * 2**20
        ),
        name="exchange",
    )(keys, values, turn_angle.T)
    out = pl.pallas_call(
        write_kernel,
        out_shape=[jax.ShapeDtypeStruct(a.shape, a.dtype) for a in arrived],
        in_specs=[vmem] * 4,
        out_specs=[anywhere] * 4,
        scratch_shapes=[pltpu.SemaphoreType.DMA((4,))],
        compiler_params=pltpu.CompilerParams(vmem_limit_bytes=2**20),
        name="write",
    )(*[pltpu.with_memory_space_constraint(a, pltpu.VMEM) for a in arrived])
    return tuple(a.reshape(per, -1, heads, size) for a in out)


def solution(mesh):
    where = P(AXES, None, "model", None)
    return jax.shard_map(
        functools.partial(on_device, mesh.shape["coarse"], mesh.shape["fine"]),
        mesh=mesh,
        in_specs=(P(None, AXES, "model", None), P(None, AXES, "model", None), P()),
        out_specs=(where, where, where, where),
        check_vma=False,
    )
```

```python
import functools

import jax
import jax.numpy as jnp
from jax import lax
from jax.experimental import pallas as pl
from jax.experimental.pallas import tpu as pltpu
from jax.sharding import PartitionSpec as P

PAGE = 32
BLOCK = 256
PIECE = 192
LAST_PIECE = 48
TILE = 16
AXES = ("coarse", "fine")
MESH = pl.DeviceIdType.MESH


def exchange_kernel(
    nc, nf, heads, keys, values, angles,
    got_keys, got_values, high, low,
    plain, turned, near_angles, cosine, sine, folded, paired,
    angle_sem, plain_sem, own_sem, key_send, key_recv, value_send, value_recv,
):
    n = nc * nf
    per, rows = keys.shape[0] // n, keys.shape[1]
    length, half = rows // heads, angles.shape[0]
    head_size = 2 * half
    mine_c, mine_f = lax.axis_index("coarse"), lax.axis_index("fine")
    me = mine_c * nf + mine_f
    my_rows = pl.ds(pl.multiple_of(me * rows, rows), rows)

    order = [(c, f) for f in range(nf) for c in range(nc)][1:]

    def device(step_c, step_f):
        c, f = lax.rem(mine_c + step_c, nc), lax.rem(mine_f + step_f, nf)
        return c, f, c * nf + f

    angle_copy = pltpu.make_async_copy(
        angles.at[:, pl.ds(pl.multiple_of(me * length, length), length)], near_angles, angle_sem
    )
    angle_copy.start()

    def chunk_of(index):
        return pl.ds(index * per, per)

    def plain_copy(slot, index):
        return pltpu.make_async_copy(keys.at[chunk_of(index)], plain.at[slot], plain_sem.at[slot])

    partners = [device(*step) for step in order]
    for slot, (_, _, index) in enumerate(partners):
        plain_copy(slot, index).start()
    plain_copy(n - 1, me).start()

    barrier = pltpu.get_barrier_semaphore()
    for c, f, _ in partners:
        pl.semaphore_signal(barrier, inc=1, device_id={"coarse": c, "fine": f}, device_id_type=MESH)
    pl.semaphore_wait(barrier, n - 1)

    def send(source, target, sends, recvs, slot, first, count):
        c, f, _ = partners[slot]
        return pltpu.make_async_remote_copy(
            src_ref=source.at[:, pl.ds(first, count)],
            dst_ref=target.at[:, pl.ds(pl.multiple_of(me * rows + first, LAST_PIECE), count)],
            send_sem=sends.at[slot],
            recv_sem=recvs.at[me],
            device_id={"coarse": c, "fine": f},
            device_id_type=MESH,
        )

    def send_values(slot, first, count):
        source = values.at[chunk_of(partners[slot][2])]
        return send(source, got_values, value_send, value_recv, slot, first, count)

    def send_keys(slot, first, count):
        return send(turned.at[slot], got_keys, key_send, key_recv, slot, first, count)

    pieces = rows // PIECE

    def send_pieces(send_one, first, last, size=PIECE):
        @pl.loop(first * (PIECE // size), last * (PIECE // size))
        def _(p):
            for slot in range(n - 1):
                send_one(slot, pl.multiple_of(p * size, size), size).start()

    send_pieces(send_values, 0, pieces // 2)
    own_copy = pltpu.make_async_copy(values.at[chunk_of(me)], got_values.at[:, my_rows], own_sem)
    own_copy.start()

    angle_copy.wait()
    cos_half = jnp.cos(near_angles[...]).T
    sin_half = jnp.sin(near_angles[...]).T
    cos_whole = jnp.concatenate([cos_half, cos_half], axis=1)
    sin_whole = jnp.concatenate([-sin_half, sin_half], axis=1)
    for h in range(heads):
        cosine[pl.ds(h, length, stride=heads), :] = cos_whole
        sine[pl.ds(h, length, stride=heads), :] = sin_whole

    def turn(slot, store):
        for s in range(per):
            @pl.loop(0, rows // BLOCK)
            def _(i):
                here = pl.ds(pl.multiple_of(i * BLOCK, BLOCK), BLOCK)
                wide = plain[slot, s, here, :].astype(jnp.float32)
                out = wide * cosine[here, :] + pltpu.roll(wide, half, 1) * sine[here, :]
                store(s, i, out.astype(jnp.bfloat16))

    def store_turned(slot):
        def store(s, i, block):
            turned[slot, s, pl.ds(pl.multiple_of(i * BLOCK, BLOCK), BLOCK), :] = block
        return store

    def store_own(s, i, block):
        got_keys[s, pl.ds(pl.multiple_of(me * rows + i * BLOCK, BLOCK), BLOCK), :] = block

    for slot, (_, _, index) in enumerate(partners):
        plain_copy(slot, index).wait()
        turn(slot, store_turned(slot))
    plain_copy(n - 1, me).wait()
    turn(n - 1, store_own)
    send_pieces(send_keys, 0, pieces)
    send_pieces(send_values, pieces // 2, pieces - 2)
    send_pieces(send_values, pieces - 2, pieces, LAST_PIECE)

    pages = length // PAGE
    fold = PAGE * heads // TILE

    def bound(index, pick, out):
        for s in range(per):
            block = got_keys[s, pl.ds(pl.multiple_of(index * rows, rows), rows), :]
            tiles = block.reshape(pages, fold, TILE, head_size)
            best = tiles[:, 0]
            for t in range(1, fold):
                best = pick(best, tiles[:, t])
            folded[...] = best.astype(jnp.float32).reshape(pages * TILE, head_size)
            for h in range(heads):
                top = folded[pl.ds(h, pages, stride=TILE), :]
                for j in range(1, TILE // heads):
                    top = pick(top, folded[pl.ds(j * heads + h, pages, stride=TILE), :])
                paired[pl.ds(h, pages, stride=heads), :] = top
            span = pages * heads
            out[s, pl.ds(pl.multiple_of(index * span, span), span), :] = paired[...].astype(jnp.bfloat16)

    bound(me, jnp.maximum, high)
    bound(me, jnp.minimum, low)

    def arrived(buffer, sems, index):
        there = buffer.at[:, pl.ds(pl.multiple_of(index * rows, rows), rows)]
        return pltpu.make_async_copy(there, there, sems.at[index])

    others = [device((nc - c) % nc, (nf - f) % nf)[2] for c, f in order]
    for index in others:
        arrived(got_keys, key_recv, index).wait()
        bound(index, jnp.maximum, high)
        bound(index, jnp.minimum, low)
    for index in others:
        arrived(got_values, value_recv, index).wait()
    own_copy.wait()
    for slot in range(n - 1):
        send_values(slot, 0, rows).wait_send()
        send_keys(slot, 0, rows).wait_send()


def write_kernel(*refs):
    count = len(refs) // 2
    sources, targets, sems = refs[:count], refs[count:2 * count], refs[2 * count]
    copies = [
        pltpu.make_async_copy(a, b, sems.at[i]) for i, (a, b) in enumerate(zip(sources, targets))
    ]
    for copy in copies:
        copy.start()
    for copy in copies:
        copy.wait()


def on_device(nc, nf, fresh_keys, fresh_values, turn_angle):
    batch, length, heads, size = fresh_keys.shape
    n, rows, half = nc * nf, length * heads, size // 2
    per = batch // n
    pages = length // PAGE
    keys = fresh_keys.reshape(batch, rows, size)
    values = fresh_values.reshape(batch, rows, size)
    whole = (per, n * rows, size)
    bounds = (per, n * pages * heads, size)
    vmem, anywhere = pl.BlockSpec(memory_space=pltpu.VMEM), pl.BlockSpec(memory_space=pl.ANY)
    arrived = pl.pallas_call(
        functools.partial(exchange_kernel, nc, nf, heads),
        out_shape=[pltpu.VMEM(shape, jnp.bfloat16) for shape in (whole, whole, bounds, bounds)],
        in_specs=[anywhere] * 3,
        out_specs=[vmem] * 4,
        scratch_shapes=[
            pltpu.VMEM((n, per, rows, size), jnp.bfloat16),
            pltpu.VMEM((n - 1, per, rows, size), jnp.bfloat16),
            pltpu.VMEM((half, length), jnp.float32),
            pltpu.VMEM((rows, size), jnp.float32),
            pltpu.VMEM((rows, size), jnp.float32),
            pltpu.VMEM((pages * TILE, size), jnp.float32),
            pltpu.VMEM((pages * heads, size), jnp.float32),
            pltpu.SemaphoreType.DMA(()),
            pltpu.SemaphoreType.DMA((n,)),
            pltpu.SemaphoreType.DMA(()),
            pltpu.SemaphoreType.DMA((n - 1,)),
            pltpu.SemaphoreType.DMA((n,)),
            pltpu.SemaphoreType.DMA((n - 1,)),
            pltpu.SemaphoreType.DMA((n,)),
        ],
        compiler_params=pltpu.CompilerParams(
            collective_id=0, has_side_effects=True, vmem_limit_bytes=40 * 2**20
        ),
        name="exchange",
    )(keys, values, turn_angle.T)
    out = pl.pallas_call(
        write_kernel,
        out_shape=[jax.ShapeDtypeStruct(a.shape, a.dtype) for a in arrived],
        in_specs=[vmem] * 4,
        out_specs=[anywhere] * 4,
        scratch_shapes=[pltpu.SemaphoreType.DMA((4,))],
        compiler_params=pltpu.CompilerParams(vmem_limit_bytes=2**20),
        name="write",
    )(*[pltpu.with_memory_space_constraint(a, pltpu.VMEM) for a in arrived])
    return tuple(a.reshape(per, -1, heads, size) for a in out)


def solution(mesh):
    where = P(AXES, None, "model", None)
    return jax.shard_map(
        functools.partial(on_device, mesh.shape["coarse"], mesh.shape["fine"]),
        mesh=mesh,
        in_specs=(P(None, AXES, "model", None), P(None, AXES, "model", None), P()),
        out_specs=(where, where, where, where),
        check_vma=False,
    )
```
